8 devices in a mesh: dp: 1 (over z), sp: 8 (over y, x, core).
Axes of the slice: x: 2, y: 2, z: 1, core: 2. Of those that a mesh axis runs over, the one named last changes fastest.
Arguments:
- hidden: bfloat16 [8, 2048, 2048], P('dp', 'sp')
- d_out: bfloat16 [8, 2048, 2048], P('dp', 'sp')
- positions: int32 [8, 2048], P('dp', 'sp')
- norm_gain: bfloat16 [2048], replicated
- w_query: bfloat16 [2048, 2048], replicated
- b_query: bfloat16 [2048], replicated
- w_key: bfloat16 [2048, 256], replicated
- b_key: bfloat16 [256], replicated
- w_value: bfloat16 [2048, 256], replicated
- b_value: bfloat16 [256], replicated
- w_out: bfloat16 [2048, 2048], replicated
Outputs:
- output 1: bfloat16 [8, 2048, 2048], P('dp', 'sp')
- output 2: bfloat16 [8, 2048, 2048], P('dp', 'sp')
- output 3: float32 [2048], P('dp')
- output 4: float32 [2048, 2048], P('dp')
- output 5: float32 [2048], P('dp')
- output 6: float32 [2048, 256], P('dp')
- output 7: float32 [256], P('dp')
- output 8: float32 [2048, 256], P('dp')
- output 9: float32 [256], P('dp')
- output 10: float32 [2048, 2048], P('dp')
All inputs are finite; a program needn't handle non-finite values.
Results may differ from the reference program's by a relative error of at most 0.02.
Values are sent between devices in bfloat16 or wider.
A program may use at most 1 GiB of HBM per device.

```python
import math
import jax
import jax.numpy as jnp
from jax import lax

D_MODEL = 2048
Q_HEADS = 16
KV_HEADS = 2
HEAD_DIM = 128
BATCH_SEQS = 8
SEQ_LEN = 2048

ROPE_BASE = 1000000.0
NORM_EPS = 1e-6


def setup_inputs(seed: int = 0, part: int = 0) -> dict:
    base_key = jax.random.key(seed)
    part_keys = jax.random.split(jax.random.fold_in(base_key, part), 4)
    shared_keys = jax.random.split(base_key, 8)
    kv_width = KV_HEADS * HEAD_DIM
    in_scale = D_MODEL ** -0.5
    act_shape = (BATCH_SEQS, SEQ_LEN, D_MODEL)
    hidden = jax.random.normal(part_keys[0], act_shape, jnp.float32)
    d_out = jax.random.normal(part_keys[1], act_shape, jnp.float32)
    pos_steps = jax.random.randint(part_keys[2], (BATCH_SEQS, SEQ_LEN), 1, 3)
    pos_starts = jax.random.randint(part_keys[3], (BATCH_SEQS, 1), 0, 1024)
    positions = jnp.cumsum(pos_steps, axis=1) - pos_steps[:, :1] + pos_starts
    norm_gain = jax.random.uniform(shared_keys[0], (D_MODEL,), jnp.float32, 0.5, 1.5)
    w_query = jax.random.normal(shared_keys[1], (D_MODEL, D_MODEL), jnp.float32) * in_scale
    b_query = jax.random.normal(shared_keys[2], (D_MODEL,), jnp.float32) * 0.3
    w_key = jax.random.normal(shared_keys[3], (D_MODEL, kv_width), jnp.float32) * in_scale
    b_key = jax.random.normal(shared_keys[4], (kv_width,), jnp.float32)
    w_value = jax.random.normal(shared_keys[5], (D_MODEL, kv_width), jnp.float32) * in_scale
    b_value = jax.random.normal(shared_keys[6], (kv_width,), jnp.float32) * 0.3
    w_out = jax.random.normal(shared_keys[7], (D_MODEL, D_MODEL), jnp.float32) * in_scale
    return dict(hidden=hidden.astype(jnp.bfloat16), d_out=d_out.astype(jnp.bfloat16),
                positions=positions.astype(jnp.int32), norm_gain=norm_gain.astype(jnp.bfloat16),
                w_query=w_query.astype(jnp.bfloat16), b_query=b_query.astype(jnp.bfloat16),
                w_key=w_key.astype(jnp.bfloat16), b_key=b_key.astype(jnp.bfloat16),
                w_value=w_value.astype(jnp.bfloat16), b_value=b_value.astype(jnp.bfloat16),
                w_out=w_out.astype(jnp.bfloat16))


def to_bf16(values_in):
    return values_in.astype(jnp.bfloat16).astype(jnp.float32)


def rope_tables(positions):
    half_dim = HEAD_DIM // 2
    inv_freq = ROPE_BASE ** (-jnp.arange(half_dim, dtype=jnp.float32) * (2.0 / HEAD_DIM))
    angles = positions.astype(jnp.float32)[..., None] * inv_freq
    return jnp.cos(angles)[:, :, None, :], jnp.sin(angles)[:, :, None, :]


def rotate(vec, cosine, sine):
    half_dim = vec.shape[-1] // 2
    first = vec[..., :half_dim]
    second = vec[..., half_dim:]
    return jnp.concatenate([first * cosine - second * sine, second * cosine + first * sine], axis=-1)


def attention(query, keys_h, values_h):
    group = Q_HEADS // KV_HEADS
    block_len = math.gcd(SEQ_LEN, max(8, (1 << 24) // (BATCH_SEQS * Q_HEADS * SEQ_LEN)))
    n_blocks = SEQ_LEN // block_len
    q_blocks = jnp.moveaxis(query.reshape(BATCH_SEQS, n_blocks, block_len, KV_HEADS, group, HEAD_DIM), 1, 0)
    key_pos = jnp.arange(SEQ_LEN)
    scale = HEAD_DIM ** -0.5

    def one_block(block_in):
        q_block, index = block_in
        scores = jnp.einsum('bqkgd,bskd->bkgqs', q_block, keys_h) * scale
        q_pos = index * block_len + jnp.arange(block_len)
        scores = jnp.where(key_pos[None, :] <= q_pos[:, None], scores, -1e30)
        probs = to_bf16(jax.nn.softmax(scores, axis=-1))
        return jnp.einsum('bkgqs,bskd->bqkgd', probs, values_h)

    out_blocks = lax.map(jax.checkpoint(one_block), (q_blocks, jnp.arange(n_blocks)))
    return jnp.moveaxis(out_blocks, 0, 1).reshape(BATCH_SEQS, SEQ_LEN, Q_HEADS, HEAD_DIM)


def reference(hidden, d_out, positions, norm_gain, w_query, b_query, w_key, b_key, w_value, b_value, w_out):
    cosine, sine = rope_tables(positions)

    def forward(x_in, gain_f, wq_f, bq_f, wk_f, bk_f, wv_f, bv_f, wo_f):
        inv_rms = lax.rsqrt(jnp.mean(x_in * x_in, axis=-1, keepdims=True) + NORM_EPS)
        normed = to_bf16(x_in * inv_rms * gain_f)
        q_pre = jnp.einsum('bsd,de->bse', normed, wq_f) + bq_f
        query = to_bf16(rotate(q_pre.reshape(BATCH_SEQS, SEQ_LEN, Q_HEADS, HEAD_DIM), cosine, sine))
        k_pre = jnp.einsum('bsd,de->bse', normed, wk_f) + bk_f
        keys_h = to_bf16(rotate(k_pre.reshape(BATCH_SEQS, SEQ_LEN, KV_HEADS, HEAD_DIM), cosine, sine))
        v_pre = jnp.einsum('bsd,de->bse', normed, wv_f) + bv_f
        values_h = to_bf16(v_pre).reshape(BATCH_SEQS, SEQ_LEN, KV_HEADS, HEAD_DIM)
        attended = to_bf16(attention(query, keys_h, values_h)).reshape(BATCH_SEQS, SEQ_LEN, D_MODEL)
        return x_in + jnp.einsum('bsd,de->bse', attended, wo_f)

    result, pullback = jax.vjp(forward, hidden.astype(jnp.float32), norm_gain.astype(jnp.float32),
                               w_query.astype(jnp.float32), b_query.astype(jnp.float32),
                               w_key.astype(jnp.float32), b_key.astype(jnp.float32),
                               w_value.astype(jnp.float32), b_value.astype(jnp.float32),
                               w_out.astype(jnp.float32))
    grads = pullback(d_out.astype(jnp.float32))
    return (result.astype(jnp.bfloat16), grads[0].astype(jnp.bfloat16), grads[1], grads[2], grads[3],
            grads[4], grads[5], grads[6], grads[7], grads[8])
```

```python
import functools
import math
import jax
import jax.numpy as jnp
from jax import lax
from jax.experimental import pallas as pl
from jax.experimental.pallas import tpu as pltpu
from jax.sharding import PartitionSpec as P

HEAD_DIM = 128
HALF = HEAD_DIM // 2
ROPE_BASE = 1000000.0
NORM_EPS = 1e-6
SCALE = HEAD_DIM ** -0.5
EXP2_SCALE = SCALE * math.log2(math.e)
MASKED = -1e30
NT_DIMS = (((1,), (1,)), ((), ()))


def dot_nt(left, right):
    return lax.dot_general(left, right, NT_DIMS, preferred_element_type=jnp.float32)


def dot_nn(left, right):
    return jnp.dot(left, right, preferred_element_type=jnp.float32)


def head_cols(head):
    return slice(head * HEAD_DIM, (head + 1) * HEAD_DIM)


def attn_fwd_kernel(index_ref, q_ref, do_ref, kv_ref, out_ref, lse_ref, delta_ref, v_t, peak, total, acc):
    index = index_ref[0]
    heads = q_ref.shape[1] // HEAD_DIM
    blocks, _, block, _ = kv_ref.shape
    pair = 2 * block

    for j in range(blocks):
        v_t[j] = kv_ref[j, 0, :, HEAD_DIM:].T
    peak[...] = jnp.full(peak.shape, MASKED, jnp.float32)
    total[...] = jnp.zeros(total.shape, jnp.float32)
    acc[...] = jnp.zeros(acc.shape, jnp.float32)

    def step(number, masked):
        keys = kv_ref[pl.ds(2 * number, 2), 0, :, :HEAD_DIM].reshape(pair, HEAD_DIM)
        if masked:
            key_pos = number * pair + lax.broadcasted_iota(jnp.int32, (pair, block), 0)
            query_pos = index * block + lax.broadcasted_iota(jnp.int32, (pair, block), 1)
            keep = key_pos <= query_pos
        scores_next = dot_nt(keys, q_ref[:, head_cols(0)])
        for h in range(heads):
            scores = scores_next
            if h + 1 < heads:
                scores_next = dot_nt(keys, q_ref[:, head_cols(h + 1)])
            if masked:
                scores = jnp.where(keep, scores, MASKED)
            old_peak = peak[h:h + 1, :]
            new_peak = jnp.maximum(old_peak, jnp.max(scores, axis=0, keepdims=True))
            alpha = jnp.exp2((old_peak - new_peak) * EXP2_SCALE)
            probs = jnp.exp2(scores * EXP2_SCALE - new_peak * EXP2_SCALE)
            total[h:h + 1, :] = alpha * total[h:h + 1, :] + jnp.sum(probs, axis=0, keepdims=True)
            peak[h:h + 1, :] = new_peak
            probs = probs.astype(jnp.bfloat16)
            update = dot_nn(v_t[2 * number], probs[:block]) + dot_nn(v_t[2 * number + 1], probs[block:])
            acc[h] = acc[h] * alpha + update

    full = index // 2

    @pl.loop(0, full)
    def _(number):
        step(number, False)

    step(full, True)

    for h in range(heads):
        out_t = (acc[h] / total[h:h + 1, :]).astype(jnp.bfloat16)
        out_ref[:, head_cols(h)] = out_t.T
        do_t = do_ref[:, head_cols(h)].T
        delta_ref[0, h:h + 1, :] = jnp.sum(out_t.astype(jnp.float32) * do_t.astype(jnp.float32), axis=0, keepdims=True)
    lse_ref[0] = peak[...] * EXP2_SCALE + jnp.log2(total[...])


def attn_bwd_kernel(index_ref, q_ref, do_ref, kv_ref, lse_ref, delta_ref, cos_ref, sin_ref,
                    dq_ref, dbq_ref, dkv_ref, dq_t):
    index = index_ref[0]
    heads = q_ref.shape[1] // HEAD_DIM
    blocks, _, block, _ = kv_ref.shape
    dq_t[...] = jnp.zeros(dq_t.shape, jnp.float32)

    def step(j, masked):
        keys = kv_ref[j, 0, :, :HEAD_DIM]
        values = kv_ref[j, 0, :, HEAD_DIM:]
        keys_t = keys.T
        d_keys = jnp.zeros((block, HEAD_DIM), jnp.float32)
        d_values = jnp.zeros((block, HEAD_DIM), jnp.float32)
        if masked:
            keep = (lax.broadcasted_iota(jnp.int32, (block, block), 0)
                    <= lax.broadcasted_iota(jnp.int32, (block, block), 1))
        for h in range(heads):
            query = q_ref[:, head_cols(h)]
            d_out = do_ref[:, head_cols(h)]
            scores = dot_nt(keys, query)
            d_probs = dot_nt(values, d_out)
            if masked:
                scores = jnp.where(keep, scores, MASKED)
            probs = jnp.exp2(scores * EXP2_SCALE - lse_ref[0, h:h + 1, :])
            d_scores = (probs * (d_probs - delta_ref[0, h:h + 1, :])).astype(jnp.bfloat16)
            d_values += dot_nn(probs.astype(jnp.bfloat16), d_out)
            d_keys += dot_nn(d_scores, query)
            dq_t[h] += dot_nn(keys_t, d_scores)
        dkv_ref[j, 0, :, :HEAD_DIM] = d_keys * SCALE
        dkv_ref[j, 0, :, HEAD_DIM:] = d_values

    @pl.loop(0, index)
    def _(j):
        step(j, False)

    step(index, True)

    @pl.loop(index + 1, blocks)
    def _(j):
        dkv_ref[j, 0] = jnp.zeros(dkv_ref.shape[2:], jnp.float32)

    @pl.when(pl.program_id(0) == 0)
    def _():
        dbq_ref[...] = jnp.zeros(dbq_ref.shape, jnp.float32)

    cosine = cos_ref[0]
    sine = sin_ref[0]
    for h in range(heads):
        first = dq_t[h, :HALF, :] * SCALE
        second = dq_t[h, HALF:, :] * SCALE
        dq_pre = jnp.concatenate([first * cosine + second * sine, second * cosine - first * sine], axis=0).T
        dbq_ref[:, head_cols(h)] += jnp.sum(dq_pre, axis=0, keepdims=True)
        dq_ref[:, head_cols(h)] = dq_pre.astype(jnp.bfloat16)


def attn_sizes(query, kv_all, kv_heads):
    blocks, batch, block, _ = kv_all.shape
    width = query.shape[1] // kv_heads
    return blocks, batch, block, width, width // HEAD_DIM


def attn_forward(index, query, d_att, kv_all, kv_head, kv_heads):
    blocks, batch, block, width, heads = attn_sizes(query, kv_all, kv_heads)
    cols = pl.BlockSpec((block, width), lambda b, _: (b, kv_head))
    stats = pl.BlockSpec((1, heads, block), lambda b, _: (b, 0, 0))
    stats_shape = jax.ShapeDtypeStruct((batch, heads, block), jnp.float32)
    grid_spec = pltpu.PrefetchScalarGridSpec(
        num_scalar_prefetch=1, grid=(batch,),
        in_specs=[cols, cols, pl.BlockSpec((blocks, 1, block, 2 * HEAD_DIM), lambda b, _: (0, b, 0, 0))],
        out_specs=[pl.BlockSpec((block, width), lambda b, _: (b, 0)), stats, stats],
        scratch_shapes=[pltpu.VMEM((blocks, HEAD_DIM, block), jnp.bfloat16),
                        pltpu.VMEM((heads, block), jnp.float32), pltpu.VMEM((heads, block), jnp.float32),
                        pltpu.VMEM((heads, HEAD_DIM, block), jnp.float32)])
    work = batch * heads * block * block * blocks
    return pl.pallas_call(
        attn_fwd_kernel, grid_spec=grid_spec,
        out_shape=[jax.ShapeDtypeStruct((batch * block, width), jnp.bfloat16), stats_shape, stats_shape],
        compiler_params=pltpu.CompilerParams(dimension_semantics=("arbitrary",)),
        cost_estimate=pl.CostEstimate(flops=8 * work * HEAD_DIM, bytes_accessed=2 ** 24, transcendentals=work),
        name="attn_fwd")(index, query, d_att, kv_all)


def attn_backward(index, query, d_att, kv_all, lse, delta, cos_t, sin_t, kv_head, kv_heads):
    blocks, batch, block, width, heads = attn_sizes(query, kv_all, kv_heads)
    cols = pl.BlockSpec((block, width), lambda b, _: (b, kv_head))
    stats = pl.BlockSpec((1, heads, block), lambda b, _: (b, 0, 0))
    table = pl.BlockSpec((1, HALF, block), lambda b, _: (b, 0, 0))
    all_keys = pl.BlockSpec((blocks, 1, block, 2 * HEAD_DIM), lambda b, _: (0, b, 0, 0))
    grid_spec = pltpu.PrefetchScalarGridSpec(
        num_scalar_prefetch=1, grid=(batch,),
        in_specs=[cols, cols, all_keys, stats, stats, table, table],
        out_specs=[pl.BlockSpec((block, width), lambda b, _: (b, 0)),
                   pl.BlockSpec((1, width), lambda b, _: (0, 0)), all_keys],
        scratch_shapes=[pltpu.VMEM((heads, HEAD_DIM, block), jnp.float32)])
    work = batch * heads * block * block * blocks
    return pl.pallas_call(
        attn_bwd_kernel, grid_spec=grid_spec,
        out_shape=[jax.ShapeDtypeStruct((batch * block, width), jnp.bfloat16),
                   jax.ShapeDtypeStruct((1, width), jnp.float32),
                   jax.ShapeDtypeStruct(kv_all.shape, jnp.float32)],
        compiler_params=pltpu.CompilerParams(dimension_semantics=("arbitrary",)),
        cost_estimate=pl.CostEstimate(flops=20 * work * HEAD_DIM, bytes_accessed=2 ** 25, transcendentals=work),
        name="attn_bwd")(index, query, d_att, kv_all, lse, delta, cos_t, sin_t)


def rotate(vec, cosine, sine):
    first = vec[..., :HALF]
    second = vec[..., HALF:]
    return jnp.concatenate([first * cosine - second * sine, second * cosine + first * sine], axis=-1)


def matmul(left, right):
    return jnp.dot(left, right, preferred_element_type=jnp.float32)


def matmul_tn(left, right):
    return lax.dot_general(left, right, (((0,), (0,)), ((), ())), preferred_element_type=jnp.float32)


def matmul_nt(left, right):
    return lax.dot_general(left, right, NT_DIMS, preferred_element_type=jnp.float32)


def solution(mesh):
    def device_step(hidden, d_out, positions, norm_gain, w_query, b_query, w_key, b_key, w_value, b_value, w_out):
        batch, tokens, d_model = hidden.shape
        rows = batch * tokens
        kv_heads = w_key.shape[1] // HEAD_DIM
        group_width = d_model // kv_heads
        index = lax.axis_index('sp').astype(jnp.int32).reshape(1)
        f32 = jnp.float32
        bf16 = jnp.bfloat16

        inv_freq = ROPE_BASE ** (-jnp.arange(HALF, dtype=f32) * (2.0 / HEAD_DIM))
        angles = positions.astype(f32)[..., None] * inv_freq
        cosine = jnp.cos(angles).reshape(rows, 1, HALF)
        sine = jnp.sin(angles).reshape(rows, 1, HALF)
        cos_t = jnp.swapaxes(cosine.reshape(batch, tokens, HALF), 1, 2)
        sin_t = jnp.swapaxes(sine.reshape(batch, tokens, HALF), 1, 2)

        x_rows = hidden.reshape(rows, d_model)
        dy_rows = d_out.reshape(rows, d_model)
        x_f = x_rows.astype(f32)
        inv_rms = lax.rsqrt(jnp.mean(x_f * x_f, axis=-1, keepdims=True) + NORM_EPS)
        gain = norm_gain.astype(f32)
        normed = (x_f * inv_rms * gain).astype(bf16)

        k_pre = (matmul(normed, w_key) + b_key.astype(f32)).reshape(rows, kv_heads, HEAD_DIM)
        keys = rotate(k_pre, cosine, sine).astype(bf16)
        values = (matmul(normed, w_value) + b_value.astype(f32)).astype(bf16).reshape(rows, kv_heads, HEAD_DIM)
        kv_all = []
        for g in range(kv_heads):
            kv = jnp.concatenate([keys[:, g], values[:, g]], axis=-1).reshape(batch, tokens, 2 * HEAD_DIM)
            kv_all.append(lax.all_gather(kv, 'sp', axis=0))

        q_pre = (matmul(normed, w_query) + b_query.astype(f32)).reshape(rows, d_model // HEAD_DIM, HEAD_DIM)
        query = rotate(q_pre, cosine, sine).astype(bf16).reshape(rows, d_model)
        d_att = matmul_nt(dy_rows, w_out).astype(bf16)

        fwd = [attn_forward(index, query, d_att, kv_all[g], g, kv_heads) for g in range(kv_heads)]
        attended = jnp.concatenate([f[0] for f in fwd], axis=1)
        block_out = (x_f + matmul(attended, w_out)).astype(bf16)
        d_w_out = lax.psum(matmul_tn(attended, dy_rows), 'sp')

        d_query, d_b_query, d_w_query, d_keys, d_values = [], [], [], [], []
        for g in range(kv_heads):
            _, lse, delta = fwd[g]
            dq, dbq, dkv = attn_backward(index, query, d_att, kv_all[g], lse, delta, cos_t, sin_t, g, kv_heads)
            dkv = lax.psum_scatter(dkv, 'sp', scatter_dimension=0).reshape(rows, 2 * HEAD_DIM)
            d_query.append(dq)
            d_b_query.append(dbq)
            d_w_query.append(lax.psum(matmul_tn(normed, dq), 'sp'))
            d_keys.append(rotate(dkv[:, :HEAD_DIM], cosine[:, 0], -sine[:, 0]))
            d_values.append(dkv[:, HEAD_DIM:])

        dk_pre = jnp.concatenate(d_keys, axis=1)
        dv_pre = jnp.concatenate(d_values, axis=1)
        dk_bf = dk_pre.astype(bf16)
        dv_bf = dv_pre.astype(bf16)
        dq_bf = jnp.concatenate(d_query, axis=1)
        d_w_key, d_w_value = lax.psum((matmul_tn(normed, dk_bf), matmul_tn(normed, dv_bf)), 'sp')
        d_normed = matmul_nt(dq_bf, w_query) + matmul_nt(dk_bf, w_key) + matmul_nt(dv_bf, w_value)
        unit = x_f * inv_rms
        d_unit = d_normed * gain
        d_input = inv_rms * (d_unit - unit * jnp.mean(d_unit * unit, axis=-1, keepdims=True))
        d_hidden = (dy_rows.astype(f32) + d_input).astype(bf16)
        d_gain, d_bq, d_bk, d_bv = lax.psum((jnp.sum(d_normed * unit, axis=0), jnp.concatenate(d_b_query, axis=1)[0],
                                             jnp.sum(dk_pre, axis=0), jnp.sum(dv_pre, axis=0)), 'sp')
        return (block_out.reshape(hidden.shape), d_hidden.reshape(hidden.shape), d_gain,
                jnp.concatenate(d_w_query, axis=1), d_bq, d_w_key, d_bk, d_w_value, d_bv, d_w_out)

    seq_spec = P('dp', 'sp', None)
    in_specs = (seq_spec, seq_spec, P('dp', 'sp'), P(), P(), P(), P(), P(), P(), P(), P())
    out_specs = (seq_spec, seq_spec, P('dp'), P('dp', None), P('dp'), P('dp', None), P('dp'),
                 P('dp', None), P('dp'), P('dp', None))
    return jax.shard_map(device_step, mesh=mesh, in_specs=in_specs, out_specs=out_specs, check_vma=False)
```
